32 devices in a mesh: dp: 1 (over z), cp: 32 (over y, x, core).
Axes of the slice: x: 4, y: 4, z: 1, core: 2. Of those that a mesh axis runs over, the one named last changes fastest.
The devices are a block of a 4x4x8 slice.
Arguments:
- x_in: bfloat16 [4096, 4096], P(('dp', 'cp'))
- dy_in: bfloat16 [4096, 4096], P(('dp', 'cp'))
- w_q: bfloat16 [4096, 4096], replicated
- w_k: bfloat16 [4096, 1024], replicated
- w_v: bfloat16 [4096, 1024], replicated
- w_o: bfloat16 [4096, 4096], replicated
Outputs:
- output 1: bfloat16 [4096, 4096], P(('dp', 'cp'))
- output 2: bfloat16 [4096, 4096], P(('dp', 'cp'))
All inputs are finite; a program needn't handle non-finite values.
Results may differ from the reference program's by a relative error of at most 0.0107204.
Values are sent between devices in bfloat16 or wider.
A program may use at most 768 MiB of HBM per device.

```python
import math
import jax
import jax.numpy as jnp
from jax import lax

SEQ_LEN = 4096
D_MODEL = 4096
Q_HEADS = 32
KV_HEADS = 8
HEAD_DIM = 128
QUERY_BLOCK = 128

Q_GROUP = Q_HEADS // KV_HEADS
SCORE_GAIN = (0.75 * math.log(SEQ_LEN)) ** 0.25


def setup_inputs(seed: int = 0, part: int = 0) -> dict:
    key_base = jax.random.key(seed)
    key_part = jax.random.fold_in(key_base, part)
    key_x, key_dy = jax.random.split(key_part)
    key_wq, key_wk, key_wv, key_wo = jax.random.split(jax.random.key(seed + 1), 4)
    in_scale = D_MODEL ** -0.5
    out_scale = (Q_HEADS * HEAD_DIM) ** -0.5
    x_in = jax.random.normal(key_x, (SEQ_LEN, D_MODEL), jnp.float32).astype(jnp.bfloat16)
    dy_in = jax.random.normal(key_dy, (SEQ_LEN, D_MODEL), jnp.float32).astype(jnp.bfloat16)
    w_q = (jax.random.normal(key_wq, (D_MODEL, Q_HEADS * HEAD_DIM), jnp.float32) * (in_scale * SCORE_GAIN)).astype(jnp.bfloat16)
    w_k = (jax.random.normal(key_wk, (D_MODEL, KV_HEADS * HEAD_DIM), jnp.float32) * (in_scale * SCORE_GAIN)).astype(jnp.bfloat16)
    w_v = (jax.random.normal(key_wv, (D_MODEL, KV_HEADS * HEAD_DIM), jnp.float32) * in_scale).astype(jnp.bfloat16)
    w_o = (jax.random.normal(key_wo, (Q_HEADS * HEAD_DIM, D_MODEL), jnp.float32) * out_scale).astype(jnp.bfloat16)
    return {"x_in": x_in, "dy_in": dy_in, "w_q": w_q, "w_k": w_k, "w_v": w_v, "w_o": w_o}


def project(rows_in, weight):
    return jnp.dot(rows_in, weight, preferred_element_type=jnp.float32).astype(jnp.bfloat16)


def reference(x_in, dy_in, w_q, w_k, w_v, w_o):
    score_scale = HEAD_DIM ** -0.5
    n_blocks = SEQ_LEN // QUERY_BLOCK
    q_rows = project(x_in, w_q).reshape(n_blocks, QUERY_BLOCK, KV_HEADS, Q_GROUP, HEAD_DIM)
    k_rows = project(x_in, w_k).reshape(SEQ_LEN, KV_HEADS, HEAD_DIM).astype(jnp.float32)
    v_rows = project(x_in, w_v).reshape(SEQ_LEN, KV_HEADS, HEAD_DIM).astype(jnp.float32)

    def forward_block(q_blk):
        q_f = q_blk.astype(jnp.float32)
        scores = jnp.einsum("thjd,uhd->thju", q_f, k_rows) * score_scale
        lse_blk = jax.nn.logsumexp(scores, axis=-1, keepdims=True)
        prob_bf = jnp.exp(scores - lse_blk).astype(jnp.bfloat16)
        out_blk = jnp.einsum("thju,uhd->thjd", prob_bf.astype(jnp.float32), v_rows).astype(jnp.bfloat16)
        return out_blk, lse_blk

    out_blocks, lse_blocks = lax.map(forward_block, q_rows)
    out_flat = out_blocks.reshape(SEQ_LEN, Q_HEADS * HEAD_DIM)
    y_out = project(out_flat, w_o)
    do_flat = jnp.dot(dy_in, w_o.T, preferred_element_type=jnp.float32).astype(jnp.bfloat16)
    do_blocks = do_flat.reshape(n_blocks, QUERY_BLOCK, KV_HEADS, Q_GROUP, HEAD_DIM)

    def backward_block(acc_pair, block_in):
        dk_acc, dv_acc = acc_pair
        q_blk, out_blk, do_blk, lse_blk = block_in
        q_f = q_blk.astype(jnp.float32)
        do_f = do_blk.astype(jnp.float32)
        scores = jnp.einsum("thjd,uhd->thju", q_f, k_rows) * score_scale
        prob_f = jnp.exp(scores - lse_blk).astype(jnp.bfloat16).astype(jnp.float32)
        row_delta = jnp.sum(do_f * out_blk.astype(jnp.float32), axis=-1, keepdims=True)
        dprob = jnp.einsum("thjd,uhd->thju", do_f, v_rows)
        dscore = (prob_f * (dprob - row_delta)).astype(jnp.bfloat16).astype(jnp.float32)
        dq_blk = (jnp.einsum("thju,uhd->thjd", dscore, k_rows) * score_scale).astype(jnp.bfloat16)
        dk_acc = dk_acc + jnp.einsum("thju,thjd->uhd", dscore, q_f) * score_scale
        dv_acc = dv_acc + jnp.einsum("thju,thjd->uhd", prob_f, do_f)
        return (dk_acc, dv_acc), dq_blk

    zero_acc = jnp.zeros((SEQ_LEN, KV_HEADS, HEAD_DIM), jnp.float32)
    acc_final, dq_blocks = lax.scan(backward_block, (zero_acc, zero_acc), (q_rows, out_blocks, do_blocks, lse_blocks))
    dq_flat = dq_blocks.reshape(SEQ_LEN, Q_HEADS * HEAD_DIM)
    dk_flat = acc_final[0].astype(jnp.bfloat16).reshape(SEQ_LEN, KV_HEADS * HEAD_DIM)
    dv_flat = acc_final[1].astype(jnp.bfloat16).reshape(SEQ_LEN, KV_HEADS * HEAD_DIM)
    dx_acc = (jnp.dot(dq_flat, w_q.T, preferred_element_type=jnp.float32)
              + jnp.dot(dk_flat, w_k.T, preferred_element_type=jnp.float32)
              + jnp.dot(dv_flat, w_v.T, preferred_element_type=jnp.float32))
    return y_out, dx_acc.astype(jnp.bfloat16)
```

```python
import functools

import jax
import jax.numpy as jnp
from jax import lax
from jax.experimental import pallas as pl
from jax.experimental.pallas import tpu as pltpu
from jax.sharding import PartitionSpec as P

HEAD_DIM = 128
LOG2E = 1.4426950408889634
N_SLOT = 4
BQ_ROWS = 512
UC_ROWS = 512
VMEM_BYTES = 62 * 1024 * 1024
MESH_ID = pl.DeviceIdType.MESH
BF = jnp.bfloat16
F32 = jnp.float32
NT = (((1,), (1,)), ((), ()))
NN = (((1,), (0,)), ((), ()))


def mm(a, b, dims=NN):
    return lax.dot_general(a, b, dims, preferred_element_type=F32)


def aligned(start, size):
    return pl.ds(pl.multiple_of(start, size), size)


def entry_barrier(seq_id, head_id, n_seq, n_head):
    sem = pltpu.get_barrier_semaphore()
    for off in range(1, n_head):
        peer = seq_id * n_head + lax.rem(head_id + off, n_head)
        pl.semaphore_signal(sem, inc=1, device_id={"cp": peer}, device_id_type=MESH_ID)
    for off in range(1, n_seq):
        peer = lax.rem(seq_id + off, n_seq) * n_head + head_id
        pl.semaphore_signal(sem, inc=1, device_id={"cp": peer}, device_id_type=MESH_ID)
    pl.semaphore_wait(sem, n_head + n_seq - 2)


def remote(src, dst, send, recv, peer):
    return pltpu.make_async_remote_copy(src_ref=src, dst_ref=dst, send_sem=send, recv_sem=recv,
                                        device_id={"cp": peer}, device_id_type=MESH_ID)


def proj_kernel(n_seq, n_head, x_ref, dy_ref, wq, wk, wv, wo, q_out, do_out, k_out, v_out,
                wbuf, obuf, q_st, do_st, k_st, v_st, w_sem, o_sem,
                q_send, q_recv, do_send, do_recv, k_send, k_recv, v_send, v_recv,
                ky_send, ky_recv, vy_send, vy_recv, loc_sem):
    me = lax.axis_index("cp")
    head_id = lax.rem(me, n_head)
    seq_id = lax.div(me, n_head)
    width = q_st.shape[2]
    per_tile = width // HEAD_DIM
    n_kv = n_head // per_tile
    n_pre = N_SLOT - 1

    def dest(step):
        return lax.rem(head_id + 1 + step, n_head)

    def col_tile(tile):
        slot = tile % N_SLOT
        if tile < n_kv:
            src = wk.at[:, pl.ds(tile * width, width)]
        elif tile < 2 * n_kv:
            src = wv.at[:, pl.ds((tile - n_kv) * width, width)]
        else:
            src = wq.at[:, aligned(dest(tile - 2 * n_kv) * width, width)]
        return pltpu.make_async_copy(src, wbuf.at[slot], w_sem.at[slot])

    def q_tile(step):
        slot = lax.rem(step + 2 * n_kv, N_SLOT)
        return pltpu.make_async_copy(wq.at[:, aligned(dest(step) * width, width)], wbuf.at[slot], w_sem.at[slot])

    def o_tile(step):
        slot = lax.rem(step, N_SLOT)
        return pltpu.make_async_copy(wo.at[aligned(dest(step) * width, width), :], obuf.at[slot], o_sem.at[slot])

    for tile in range(n_pre):
        col_tile(tile).start()
    entry_barrier(seq_id, head_id, n_seq, n_head)

    def kv_send(tile):
        stage, out, send, recv, loc = (k_st, k_out, k_send, k_recv, 0) if tile < n_kv else (v_st, v_out, v_send, v_recv, 1)
        for sub in range(per_tile):
            head = (tile % n_kv) * per_tile + sub

            @pl.when(head != head_id)
            def _():
                remote(stage.at[head], out.at[me], send.at[head], recv.at[head_id], seq_id * n_head + head).start()

            @pl.when(head == head_id)
            def _():
                pltpu.make_async_copy(stage.at[head], out.at[me], loc_sem.at[loc]).start()

    for tile in range(2 * n_kv):
        col_tile(tile).wait()
        if tile >= 1:
            kv_send(tile - 1)
        col_tile(tile + n_pre).start()
        prod = mm(x_ref[...], wbuf[tile % N_SLOT]).astype(BF)
        stage = k_st if tile < n_kv else v_st
        for sub in range(per_tile):
            stage[(tile % n_kv) * per_tile + sub] = prod[:, sub * HEAD_DIM:(sub + 1) * HEAD_DIM]

    def send_piece(stage, out, send, recv, loc, step):
        head = dest(step)

        @pl.when(step < n_head - 1)
        def _():
            remote(stage.at[head], out.at[head_id], send.at[head], recv.at[head_id], seq_id * n_head + head).start()

        @pl.when(step == n_head - 1)
        def _():
            pltpu.make_async_copy(stage.at[head], out.at[head_id], loc_sem.at[loc]).start()

    def row_copy(stage, out, send, recv, off, dst_base):
        src = lax.rem(head_id + off, n_head)
        return remote(stage.at[src], out.at[dst_base + src], send.at[src], recv.at[src], seq_id * n_head + src)

    def relay_copy(out, send, recv, off):
        rows = pl.ds(seq_id * n_head, n_head)
        peer = lax.rem(seq_id + off, n_seq) * n_head + head_id
        return remote(out.at[rows], out.at[rows], send.at[off - 1], recv.at[off - 1], peer)

    relay_step = n_head // 2

    def q_step(step, carry):
        q_tile(step).wait()

        @pl.when(step == 0)
        def _():
            kv_send(2 * n_kv - 1)

        @pl.when(step > 0)
        def _():
            send_piece(q_st, q_out, q_send, q_recv, 2, step - 1)

        @pl.when(step + n_pre < n_head)
        def _():
            q_tile(step + n_pre).start()

        @pl.when(step + n_pre >= n_head)
        def _():
            o_tile(step + n_pre - n_head).start()

        @pl.when(step == relay_step)
        def _():
            for stage, out, send, recv, loc in ((k_st, k_out, k_send, k_recv, 0), (v_st, v_out, v_send, v_recv, 1)):
                for off in range(1, n_head):
                    row_copy(stage, out, send, recv, off, seq_id * n_head).wait_recv()
                pltpu.make_async_copy(stage.at[head_id], out.at[me], loc_sem.at[loc]).wait()
            for off in range(1, n_seq):
                relay_copy(k_out, ky_send, ky_recv, off).start()
                relay_copy(v_out, vy_send, vy_recv, off).start()

        slot = lax.rem(step + 2 * n_kv, N_SLOT)
        q_st[dest(step)] = mm(x_ref[...], wbuf[slot]).astype(BF)
        return carry

    lax.fori_loop(0, n_head, q_step, 0)

    def do_step(step, carry):
        o_tile(step).wait()

        @pl.when(step == 0)
        def _():
            send_piece(q_st, q_out, q_send, q_recv, 2, n_head - 1)

        @pl.when(step > 0)
        def _():
            send_piece(do_st, do_out, do_send, do_recv, 3, step - 1)

        @pl.when(step + n_pre < n_head)
        def _():
            o_tile(step + n_pre).start()

        do_st[dest(step)] = mm(dy_ref[...], obuf[lax.rem(step, N_SLOT)], NT).astype(BF)
        return carry

    lax.fori_loop(0, n_head, do_step, 0)
    for off in range(1, n_head):
        row_copy(q_st, q_out, q_send, q_recv, off, 0).wait_recv()
    pltpu.make_async_copy(q_st.at[head_id], q_out.at[head_id], loc_sem.at[2]).wait()
    send_piece(do_st, do_out, do_send, do_recv, 3, n_head - 1)
    for off in range(1, n_head):
        row_copy(k_st, k_out, k_send, k_recv, off, seq_id * n_head).wait_send()
        row_copy(v_st, v_out, v_send, v_recv, off, seq_id * n_head).wait_send()
        row_copy(q_st, q_out, q_send, q_recv, off, 0).wait_send()
        row_copy(do_st, do_out, do_send, do_recv, off, 0).wait()
    for off in range(1, n_seq):
        for out, send, recv in ((k_out, ky_send, ky_recv), (v_out, vy_send, vy_recv)):
            relay_copy(out, send, recv, off).wait_send()
            rows = pl.ds(lax.rem(seq_id + n_seq - off, n_seq) * n_head, n_head)
            remote(out.at[rows], out.at[rows], send.at[off - 1], recv.at[off - 1], me).wait_recv()
    pltpu.make_async_copy(do_st.at[head_id], do_out.at[head_id], loc_sem.at[3]).wait()


def attend_kernel(q_ref, do_ref, k_ref, v_ref, o_ref, dq_ref, dk_ref, dv_ref, kt, vt, s_buf, p_buf):
    n_keys = k_ref.shape[0]
    rows = q_ref.shape[0] * q_ref.shape[1]
    blk = min(UC_ROWS, n_keys)
    n_blk = n_keys // blk
    scale = HEAD_DIM ** -0.5
    gain = scale * LOG2E

    @pl.when((pl.program_id(0) == 0) & (pl.program_id(1) == 0))
    def _():
        def prep(i, carry):
            part = aligned(i * blk, blk)
            kt[:, part] = k_ref[part, :].astype(F32).T.astype(BF)
            vt[:, part] = v_ref[part, :].astype(F32).T.astype(BF)
            dk_ref[part, :] = jnp.zeros((blk, HEAD_DIM), F32)
            dv_ref[part, :] = jnp.zeros((blk, HEAD_DIM), F32)
            return carry
        lax.fori_loop(0, n_blk, prep, 0)

    q_blk = q_ref[...].reshape(rows, HEAD_DIM)
    do_blk = do_ref[...].reshape(rows, HEAD_DIM)

    def score(i, top):
        part = aligned(i * blk, blk)
        s = mm(k_ref[part, :], q_blk, NT)
        s_buf[part, :] = s
        return jnp.maximum(top, jnp.max(s.reshape(blk // 8, 8, rows), axis=0))

    top = lax.fori_loop(0, n_blk, score, jnp.full((8, rows), -jnp.inf, F32))
    top = jnp.max(top, axis=0, keepdims=True)

    def expo(i, tot):
        part = aligned(i * blk, blk)
        e = jnp.exp2((s_buf[part, :] - top) * gain)
        s_buf[part, :] = e
        return tot + jnp.sum(e.reshape(blk // 8, 8, rows), axis=0)

    tot = lax.fori_loop(0, n_blk, expo, jnp.zeros((8, rows), F32))
    inv = 1.0 / jnp.sum(tot, axis=0, keepdims=True)

    def value(i, acc):
        part = aligned(i * blk, blk)
        p = (s_buf[part, :] * inv).astype(BF)
        p_buf[part, :] = p
        return acc + mm(vt[:, part], p)

    out_t = lax.fori_loop(0, n_blk, value, jnp.zeros((HEAD_DIM, rows), F32)).astype(BF).astype(F32)
    o_ref[...] = out_t.T.astype(BF).reshape(o_ref.shape)
    delta = jnp.sum(do_blk.astype(F32).T * out_t, axis=0, keepdims=True)

    def grad(i, acc):
        part = aligned(i * blk, blk)
        p = p_buf[part, :]
        dp = mm(v_ref[part, :], do_blk, NT)
        ds = (p.astype(F32) * (dp - delta)).astype(BF)
        dv_ref[part, :] += mm(p, do_blk)
        dk_ref[part, :] += mm(ds, q_blk)
        return acc + mm(kt[:, part], ds)

    dq_t = lax.fori_loop(0, n_blk, grad, jnp.zeros((HEAD_DIM, rows), F32)) * scale
    dq_ref[...] = dq_t.T.astype(BF).reshape(dq_ref.shape)


def out_kernel(n_seq, n_head, o_in, dq_in, dk_in, dv_in, wq, wk, wv, wo, y_ref, dx_ref,
               wbuf, rbuf, wk_buf, wv_buf, o_full, dq_full, acc, own_k, own_v, rx_k, rx_v, k_st, v_st, dk_full, dv_full,
               w_sem, r_sem, kv_sem, o_send, o_recv, dq_send, dq_recv, yk_send, yk_recv, yv_send, yv_recv,
               k_send, k_recv, v_send, v_recv, loc_sem):
    me = lax.axis_index("cp")
    head_id = lax.rem(me, n_head)
    seq_id = lax.div(me, n_head)
    n_rows = y_ref.shape[0]
    width = o_in.shape[2]
    tile = wbuf.shape[2]
    n_tile = y_ref.shape[1] // tile
    n_pre = N_SLOT - 1

    def col_tile(step):
        slot = lax.rem(step, N_SLOT)
        return pltpu.make_async_copy(wo.at[:, aligned(step * tile, tile)], wbuf.at[slot], w_sem.at[slot])

    def row_tile(step):
        slot = lax.rem(step, N_SLOT)
        return pltpu.make_async_copy(wq.at[aligned(step * tile, tile), :], rbuf.at[slot], r_sem.at[slot])

    wide = aligned(head_id * width, width)
    slim = aligned(head_id * HEAD_DIM, HEAD_DIM)
    local_copies = (
        pltpu.make_async_copy(o_in.at[head_id], o_full.at[:, wide], loc_sem.at[0]),
        pltpu.make_async_copy(dq_in.at[head_id], dq_full.at[:, wide], loc_sem.at[1]),
        pltpu.make_async_copy(dk_in.at[seq_id], own_k, loc_sem.at[2]),
        pltpu.make_async_copy(dv_in.at[seq_id], own_v, loc_sem.at[3]),
    )
    for copy in local_copies:
        copy.start()
    for step in range(n_pre):
        col_tile(step).start()
    entry_barrier(seq_id, head_id, n_seq, n_head)

    def seq_copy(src, rx, send, recv, off):
        peer_seq = lax.rem(seq_id + off, n_seq)
        return remote(src.at[peer_seq], rx.at[off - 1], send.at[off - 1], recv.at[off - 1], peer_seq * n_head + head_id)

    def row_copy(src, dst, cols, send, recv, off):
        head = lax.rem(head_id + off, n_head)
        return remote(src.at[head], dst.at[:, cols], send.at[off - 1], recv.at[off - 1], seq_id * n_head + head)

    for off in range(1, n_seq):
        seq_copy(dk_in, rx_k, yk_send, yk_recv, off).start()
    for off in range(1, n_seq):
        seq_copy(dv_in, rx_v, yv_send, yv_recv, off).start()
    for off in range(1, n_head):
        row_copy(o_in, o_full, wide, o_send, o_recv, off).start()
    for off in range(1, n_head):
        row_copy(dq_in, dq_full, wide, dq_send, dq_recv, off).start()

    def arrived(src, dst, size, send, recv, off):
        head = lax.rem(head_id + n_head - off, n_head)
        remote(src.at[head], dst.at[:, aligned(head * size, size)], send.at[off - 1], recv.at[off - 1], me).wait_recv()

    for off in range(1, n_head):
        arrived(o_in, o_full, width, o_send, o_recv, off)
    local_copies[0].wait()

    def y_step(step, carry):
        col_tile(step).wait()

        @pl.when(step + n_pre < n_tile)
        def _():
            col_tile(step + n_pre).start()

        @pl.when(step + n_pre >= n_tile)
        def _():
            row_tile(step + n_pre - n_tile).start()

        y_ref[:, aligned(step * tile, tile)] = mm(o_full[...], wbuf[lax.rem(step, N_SLOT)]).astype(BF)
        return carry

    lax.fori_loop(0, n_tile, y_step, 0)
    for off in range(1, n_head):
        arrived(dq_in, dq_full, width, dq_send, dq_recv, off)
    local_copies[1].wait()
    kv_copies = (pltpu.make_async_copy(wk, wk_buf, kv_sem.at[0]), pltpu.make_async_copy(wv, wv_buf, kv_sem.at[1]))

    def dx_step(step, carry):
        row_tile(step).wait()

        @pl.when(step + n_pre < n_tile)
        def _():
            row_tile(step + n_pre).start()

        @pl.when(step + n_pre == n_tile)
        def _():
            kv_copies[0].start()
            kv_copies[1].start()

        acc[:, aligned(step * tile, tile)] = mm(dq_full[...], rbuf[lax.rem(step, N_SLOT)], NT)
        return carry

    lax.fori_loop(0, n_tile, dx_step, 0)
    scale = HEAD_DIM ** -0.5

    def reduce_own(src, own, rx, stage, send, recv, copy, gain):
        copy.wait()
        for off in range(1, n_seq):
            remote(src.at[seq_id], rx.at[off - 1], send.at[off - 1], recv.at[off - 1], me).wait_recv()

        def one(head, carry):
            rows = aligned(head * n_rows, n_rows)
            total = own[rows, :]
            for off in range(1, n_seq):
                total = total + rx[off - 1, rows, :]
            stage[head] = (total * gain).astype(BF)
            return carry

        lax.fori_loop(0, n_head, one, 0)

    reduce_own(dk_in, own_k, rx_k, k_st, yk_send, yk_recv, local_copies[2], scale)
    reduce_own(dv_in, own_v, rx_v, v_st, yv_send, yv_recv, local_copies[3], 1.0)
    for off in range(1, n_head):
        row_copy(k_st, dk_full, slim, k_send, k_recv, off).start()
    for off in range(1, n_head):
        row_copy(v_st, dv_full, slim, v_send, v_recv, off).start()
    dk_full[:, slim] = k_st[head_id]
    dv_full[:, slim] = v_st[head_id]
    for copy in kv_copies:
        copy.wait()
    for off in range(1, n_head):
        arrived(k_st, dk_full, HEAD_DIM, k_send, k_recv, off)
    for off in range(1, n_head):
        arrived(v_st, dv_full, HEAD_DIM, v_send, v_recv, off)

    def last_step(step, carry):
        part = aligned(step * tile, tile)
        total = acc[:, part] + mm(dk_full[...], wk_buf[part, :], NT) + mm(dv_full[...], wv_buf[part, :], NT)
        dx_ref[:, part] = total.astype(BF)
        return carry

    lax.fori_loop(0, n_tile, last_step, 0)
    for off in range(1, n_seq):
        seq_copy(dk_in, rx_k, yk_send, yk_recv, off).wait_send()
        seq_copy(dv_in, rx_v, yv_send, yv_recv, off).wait_send()
    for off in range(1, n_head):
        row_copy(o_in, o_full, wide, o_send, o_recv, off).wait_send()
        row_copy(dq_in, dq_full, wide, dq_send, dq_recv, off).wait_send()
        row_copy(k_st, dk_full, slim, k_send, k_recv, off).wait_send()
        row_copy(v_st, dv_full, slim, v_send, v_recv, off).wait_send()


def solution(mesh):
    n_group = mesh.shape["cp"]
    row_spec = P(("dp", "cp"), None)
    full_spec = P(None, None)
    any_spec = pl.BlockSpec(memory_space=pl.ANY)
    vmem_spec = pl.BlockSpec(memory_space=pltpu.VMEM)
    dma = pltpu.SemaphoreType.DMA

    def local_body(x_loc, dy_loc, w_q, w_k, w_v, w_o):
        n_rows, n_model = x_loc.shape
        n_head = w_k.shape[1] // HEAD_DIM
        width = w_q.shape[1] // n_head
        q_group = width // HEAD_DIM
        n_seq = n_group // n_head
        n_keys = n_rows * n_group
        tile = width

        q_all, do_all, k_all, v_all = pl.pallas_call(
            functools.partial(proj_kernel, n_seq, n_head),
            out_shape=(jax.ShapeDtypeStruct((n_head, n_rows, width), BF), jax.ShapeDtypeStruct((n_head, n_rows, width), BF),
                       jax.ShapeDtypeStruct((n_group, n_rows, HEAD_DIM), BF), jax.ShapeDtypeStruct((n_group, n_rows, HEAD_DIM), BF)),
            in_specs=[vmem_spec, vmem_spec] + [any_spec] * 4,
            out_specs=(any_spec,) * 4,
            scratch_shapes=[pltpu.VMEM((N_SLOT, n_model, width), BF), pltpu.VMEM((N_SLOT, width, n_model), BF),
                            pltpu.VMEM((n_head, n_rows, width), BF), pltpu.VMEM((n_head, n_rows, width), BF),
                            pltpu.VMEM((n_head, n_rows, HEAD_DIM), BF), pltpu.VMEM((n_head, n_rows, HEAD_DIM), BF),
                            dma((N_SLOT,)), dma((N_SLOT,))]
                           + [dma((n_head,))] * 8 + [dma((n_seq - 1,))] * 4 + [dma((4,))],
            compiler_params=pltpu.CompilerParams(collective_id=0, has_side_effects=True, vmem_limit_bytes=VMEM_BYTES),
            name="proj_scatter",
        )(x_loc, dy_loc, w_q, w_k, w_v, w_o)

        n_src = max(1, min(n_head, BQ_ROWS // n_rows))
        rows = n_src * n_rows
        blk_spec = pl.BlockSpec((n_src, n_rows, HEAD_DIM), lambda j, b: (b, 0, j))
        key_spec = pl.BlockSpec((n_keys, HEAD_DIM), lambda j, b: (0, 0))
        o_blk, dq_blk, dk_part, dv_part = pl.pallas_call(
            attend_kernel,
            grid=(q_group, n_head // n_src),
            out_shape=(jax.ShapeDtypeStruct((n_head, n_rows, width), BF), jax.ShapeDtypeStruct((n_head, n_rows, width), BF),
                       jax.ShapeDtypeStruct((n_keys, HEAD_DIM), F32), jax.ShapeDtypeStruct((n_keys, HEAD_DIM), F32)),
            in_specs=[blk_spec, blk_spec, key_spec, key_spec],
            out_specs=(blk_spec, blk_spec, key_spec, key_spec),
            scratch_shapes=[pltpu.VMEM((HEAD_DIM, n_keys), BF), pltpu.VMEM((HEAD_DIM, n_keys), BF),
                            pltpu.VMEM((n_keys, rows), F32), pltpu.VMEM((n_keys, rows), BF)],
            compiler_params=pltpu.CompilerParams(dimension_semantics=("arbitrary", "arbitrary"), vmem_limit_bytes=VMEM_BYTES),
            name="attend",
        )(q_all, do_all, k_all.reshape(n_keys, HEAD_DIM), v_all.reshape(n_keys, HEAD_DIM))

        seq_rows = n_head * n_rows
        part_shape = (n_seq, seq_rows, HEAD_DIM)
        y_loc, dx_loc = pl.pallas_call(
            functools.partial(out_kernel, n_seq, n_head),
            out_shape=(jax.ShapeDtypeStruct((n_rows, n_model), BF), jax.ShapeDtypeStruct((n_rows, n_model), BF)),
            in_specs=[any_spec] * 8,
            out_specs=(vmem_spec, vmem_spec),
            scratch_shapes=[pltpu.VMEM((N_SLOT, w_o.shape[0], tile), BF), pltpu.VMEM((N_SLOT, tile, w_q.shape[1]), BF),
                            pltpu.VMEM(w_k.shape, BF), pltpu.VMEM(w_v.shape, BF),
                            pltpu.VMEM((n_rows, w_q.shape[1]), BF), pltpu.VMEM((n_rows, w_q.shape[1]), BF),
                            pltpu.VMEM((n_rows, n_model), F32),
                            pltpu.VMEM((seq_rows, HEAD_DIM), F32), pltpu.VMEM((seq_rows, HEAD_DIM), F32),
                            pltpu.VMEM((n_seq - 1, seq_rows, HEAD_DIM), F32), pltpu.VMEM((n_seq - 1, seq_rows, HEAD_DIM), F32),
                            pltpu.VMEM((n_head, n_rows, HEAD_DIM), BF), pltpu.VMEM((n_head, n_rows, HEAD_DIM), BF),
                            pltpu.VMEM((n_rows, w_k.shape[1]), BF), pltpu.VMEM((n_rows, w_v.shape[1]), BF),
                            dma((N_SLOT,)), dma((N_SLOT,)), dma((2,))]
                           + [dma((n_head - 1,))] * 4 + [dma((n_seq - 1,))] * 4 + [dma((n_head - 1,))] * 4 + [dma((4,))],
            compiler_params=pltpu.CompilerParams(collective_id=1, has_side_effects=True, vmem_limit_bytes=VMEM_BYTES),
            name="gather_out",
        )(o_blk, dq_blk, dk_part.reshape(part_shape), dv_part.reshape(part_shape), w_q, w_k, w_v, w_o)
        return y_loc, dx_loc

    return jax.shard_map(local_body, mesh=mesh,
                         in_specs=(row_spec, row_spec, full_spec, full_spec, full_spec, full_spec),
                         out_specs=(row_spec, row_spec), check_vma=False)
```

```python
import functools

import jax
import jax.numpy as jnp
from jax import lax
from jax.experimental import pallas as pl
from jax.experimental.pallas import tpu as pltpu
from jax.sharding import PartitionSpec as P

HEAD_DIM = 128
LOG2E = 1.4426950408889634
N_SLOT = 4
BQ_ROWS = 512
UC_ROWS = 512
VMEM_BYTES = 62 * 1024 * 1024
VMEM_MAIN = 67000000
MESH_ID = pl.DeviceIdType.MESH
BF = jnp.bfloat16
F32 = jnp.float32
NT = (((1,), (1,)), ((), ()))
NN = (((1,), (0,)), ((), ()))


def mm(a, b, dims=NN):
    return lax.dot_general(a, b, dims, preferred_element_type=F32)


def aligned(start, size):
    return pl.ds(pl.multiple_of(start, size), size)


def entry_barrier(seq_id, head_id, n_seq, n_head):
    sem = pltpu.get_barrier_semaphore()
    for off in range(1, n_head):
        peer = seq_id * n_head + lax.rem(head_id + off, n_head)
        pl.semaphore_signal(sem, inc=1, device_id={"cp": peer}, device_id_type=MESH_ID)
    for off in range(1, n_seq):
        peer = lax.rem(seq_id + off, n_seq) * n_head + head_id
        pl.semaphore_signal(sem, inc=1, device_id={"cp": peer}, device_id_type=MESH_ID)
    pl.semaphore_wait(sem, n_head + n_seq - 2)


def remote(src, dst, send, recv, peer):
    return pltpu.make_async_remote_copy(src_ref=src, dst_ref=dst, send_sem=send, recv_sem=recv,
                                        device_id={"cp": peer}, device_id_type=MESH_ID)


def proj_kernel(n_seq, n_head, x_ref, dy_ref, wq, wk, wv, wo, q_out, do_out, k_out, v_out,
                wbuf, obuf, q_st, k_st, v_st, w_sem, o_sem,
                q_send, q_recv, k_send, k_recv, v_send, v_recv,
                ky_send, ky_recv, vy_send, vy_recv, loc_sem):
    me = lax.axis_index("cp")
    head_id = lax.rem(me, n_head)
    seq_id = lax.div(me, n_head)
    width = q_st.shape[2]
    per_tile = width // HEAD_DIM
    n_kv = n_head // per_tile
    n_pre = N_SLOT - 1

    def dest(step):
        return lax.rem(head_id + 1 + step, n_head)

    def col_tile(tile):
        slot = tile % N_SLOT
        if tile < n_kv:
            src = wk.at[:, pl.ds(tile * width, width)]
        elif tile < 2 * n_kv:
            src = wv.at[:, pl.ds((tile - n_kv) * width, width)]
        else:
            src = wq.at[:, aligned(dest(tile - 2 * n_kv) * width, width)]
        return pltpu.make_async_copy(src, wbuf.at[slot], w_sem.at[slot])

    def q_tile(step):
        slot = lax.rem(step + 2 * n_kv, N_SLOT)
        return pltpu.make_async_copy(wq.at[:, aligned(dest(step) * width, width)], wbuf.at[slot], w_sem.at[slot])

    def o_tile(step):
        slot = lax.rem(step, N_SLOT)
        return pltpu.make_async_copy(wo.at[aligned(dest(step) * width, width), :], obuf.at[slot], o_sem.at[slot])

    for tile in range(n_pre):
        col_tile(tile).start()
    entry_barrier(seq_id, head_id, n_seq, n_head)

    def kv_send(tile):
        stage, out, send, recv, loc = (k_st, k_out, k_send, k_recv, 0) if tile < n_kv else (v_st, v_out, v_send, v_recv, 1)
        for sub in range(per_tile):
            head = (tile % n_kv) * per_tile + sub

            @pl.when(head != head_id)
            def _():
                remote(stage.at[head], out.at[me], send.at[head], recv.at[head_id], seq_id * n_head + head).start()

            @pl.when(head == head_id)
            def _():
                pltpu.make_async_copy(stage.at[head], out.at[me], loc_sem.at[loc]).start()

    for tile in range(2 * n_kv):
        col_tile(tile).wait()
        if tile >= 1:
            kv_send(tile - 1)
        col_tile(tile + n_pre).start()
        prod = mm(x_ref[...], wbuf[tile % N_SLOT]).astype(BF)
        stage = k_st if tile < n_kv else v_st
        for sub in range(per_tile):
            stage[(tile % n_kv) * per_tile + sub] = prod[:, sub * HEAD_DIM:(sub + 1) * HEAD_DIM]

    def send_piece(stage, out, send, recv, loc, step):
        head = dest(step)

        @pl.when(step < n_head - 1)
        def _():
            remote(stage.at[head], out.at[head_id], send.at[head], recv.at[head_id], seq_id * n_head + head).start()

        @pl.when(step == n_head - 1)
        def _():
            pltpu.make_async_copy(stage.at[head], out.at[head_id], loc_sem.at[loc]).start()

    def row_copy(stage, out, send, recv, off, dst_base):
        src = lax.rem(head_id + off, n_head)
        return remote(stage.at[src], out.at[dst_base + src], send.at[src], recv.at[src], seq_id * n_head + src)

    ahead, behind = 1, n_seq - 1

    def seq_copy(out, send, recv, slot, origin, off):
        rows = pl.ds(lax.rem(seq_id + origin, n_seq) * n_head, n_head)
        peer = lax.rem(seq_id + off, n_seq) * n_head + head_id
        return remote(out.at[rows], out.at[rows], send.at[slot], recv.at[slot], peer)

    relays = ((k_out, ky_send, ky_recv, ahead), (v_out, vy_send, vy_recv, behind))

    def forward():
        for out, send, recv, off in relays:
            seq_copy(out, send, recv, 0, n_seq - off, off).wait_recv()
            seq_copy(out, send, recv, 2, n_seq - off, off).start()

    relay_step = n_head // 2

    def q_step(step, carry):
        q_tile(step).wait()

        @pl.when(step == 0)
        def _():
            kv_send(2 * n_kv - 1)

        @pl.when(step > 0)
        def _():
            send_piece(q_st, q_out, q_send, q_recv, 2, step - 1)

        @pl.when(step + n_pre < n_head)
        def _():
            q_tile(step + n_pre).start()

        @pl.when(step + n_pre >= n_head)
        def _():
            o_tile(step + n_pre - n_head).start()

        @pl.when(step == relay_step)
        def _():
            for stage, out, send, recv, loc in ((k_st, k_out, k_send, k_recv, 0), (v_st, v_out, v_send, v_recv, 1)):
                for off in range(1, n_head):
                    row_copy(stage, out, send, recv, off, seq_id * n_head).wait_recv()
                pltpu.make_async_copy(stage.at[head_id], out.at[me], loc_sem.at[loc]).wait()
            for out, send, recv, off in relays:
                seq_copy(out, send, recv, 0, 0, off).start()
                seq_copy(out, send, recv, 1, 0, n_seq - off).start()

        slot = lax.rem(step + 2 * n_kv, N_SLOT)
        q_st[dest(step)] = mm(x_ref[...], wbuf[slot]).astype(BF)
        return carry

    lax.fori_loop(0, n_head, q_step, 0)

    forward_step = (5 * n_head) // 8

    def do_step(step, carry):
        o_tile(step).wait()

        @pl.when(step == 0)
        def _():
            send_piece(q_st, q_out, q_send, q_recv, 2, n_head - 1)

        @pl.when(step == forward_step)
        def _():
            forward()

        @pl.when(step + n_pre < n_head)
        def _():
            o_tile(step + n_pre).start()

        do_out[dest(step)] = mm(dy_ref[...], obuf[lax.rem(step, N_SLOT)], NT).astype(BF)
        return carry

    lax.fori_loop(0, n_head, do_step, 0)
    for off in range(1, n_head):
        row_copy(q_st, q_out, q_send, q_recv, off, 0).wait()
        row_copy(k_st, k_out, k_send, k_recv, off, seq_id * n_head).wait_send()
        row_copy(v_st, v_out, v_send, v_recv, off, seq_id * n_head).wait_send()
    pltpu.make_async_copy(q_st.at[head_id], q_out.at[head_id], loc_sem.at[2]).wait()
    for out, send, recv, off in relays:
        seq_copy(out, send, recv, 0, 0, off).wait_send()
        seq_copy(out, send, recv, 1, 0, n_seq - off).wait_send()
        seq_copy(out, send, recv, 2, n_seq - off, off).wait_send()
        seq_copy(out, send, recv, 1, off, off).wait_recv()
        seq_copy(out, send, recv, 2, 2, off).wait_recv()


def main_kernel(n_seq, n_head, q_in, do_in, k_in, v_in, wq, wk, wv, wo, y_ref, dx_ref,
                p_all, s_buf, q_vm, k_vm, v_vm, kt, vt, do_vm, o_vm, dq_vm, o_full, dq_full, delta_ref,
                dk_acc, dv_acc, mid_k, mid_v, rx_k, rx_v, k_st, v_st, dk_full, dv_full,
                in_sem, w_sem, loc_sem, do_send, do_recv, o_send, o_recv, dq_send, dq_recv,
                k_send, k_recv, v_send, v_recv, yk_send, yk_recv, yv_send, yv_recv):
    me = lax.axis_index("cp")
    head_id = lax.rem(me, n_head)
    seq_id = lax.div(me, n_head)
    n_keys = k_vm.shape[0]
    n_rows, width = q_vm.shape[1], q_vm.shape[2]
    q_group = width // HEAD_DIM
    n_step, _, rows = p_all.shape
    n_src = rows // n_rows
    n_blk = n_step // q_group
    tile = p_all.shape[2]
    n_tile = y_ref.shape[1] // tile
    blk = min(UC_ROWS, n_keys // n_seq)
    n_chunk = n_keys // blk
    part_keys = n_keys // n_seq
    scale = HEAD_DIM ** -0.5
    gain = scale * LOG2E
    ahead, behind = 1, n_seq - 1

    def row_peer(off):
        return lax.rem(head_id + off, n_head)

    def row_copy(src, dst, send, recv, off):
        return remote(src.at[row_peer(off)], dst, send.at[off - 1], recv.at[off - 1], seq_id * n_head + row_peer(off))

    def col_copy(src, dst, send, recv, slot, off):
        return remote(src, dst, send.at[slot], recv.at[slot], lax.rem(seq_id + off, n_seq) * n_head + head_id)

    wide = aligned(head_id * width, width)
    slim = aligned(head_id * HEAD_DIM, HEAD_DIM)

    def from_peer(off):
        return row_peer(n_head - off)

    loads = (pltpu.make_async_copy(k_in, k_vm, in_sem.at[0]), pltpu.make_async_copy(q_in, q_vm, in_sem.at[1]),
             pltpu.make_async_copy(v_in, v_vm, in_sem.at[2]),
             pltpu.make_async_copy(do_in.at[head_id], do_vm.at[head_id], in_sem.at[3]))
    for copy in loads:
        copy.start()
    entry_barrier(seq_id, head_id, n_seq, n_head)
    for off in range(1, n_head):
        row_copy(do_in, do_vm.at[head_id], do_send, do_recv, off).start()
    for copy in loads[:3]:
        copy.wait()

    def prep(i, carry):
        part = aligned(i * blk, blk)
        kt[:, part] = k_vm[part, :].astype(F32).T.astype(BF)
        vt[:, part] = v_vm[part, :].astype(F32).T.astype(BF)
        return carry

    lax.fori_loop(0, n_chunk, prep, 0)

    def block_of(step):
        return pl.ds(lax.rem(step, n_blk) * n_src, n_src), aligned(lax.div(step, n_blk) * HEAD_DIM, HEAD_DIM)

    def read_block(ref, step):
        srcs, cols = block_of(step)
        return ref[srcs, :, cols].reshape(rows, HEAD_DIM)

    def forward(step, carry):
        q_blk = read_block(q_vm, step)

        def score(i, top):
            part = aligned(i * blk, blk)
            s = mm(k_vm[part, :], q_blk, NT)
            s_buf[part, :] = s
            return jnp.maximum(top, jnp.max(s.reshape(blk // 8, 8, rows), axis=0))

        top = lax.fori_loop(0, n_chunk, score, jnp.full((8, rows), -jnp.inf, F32))
        top = jnp.max(top, axis=0, keepdims=True)

        def expo(i, tot):
            part = aligned(i * blk, blk)
            e = jnp.exp2((s_buf[part, :] - top) * gain)
            s_buf[part, :] = e
            return tot + jnp.sum(e.reshape(blk // 8, 8, rows), axis=0)

        tot = lax.fori_loop(0, n_chunk, expo, jnp.zeros((8, rows), F32))
        inv = 1.0 / jnp.sum(tot, axis=0, keepdims=True)

        def value(i, acc):
            part = aligned(i * blk, blk)
            p = (s_buf[part, :] * inv).astype(BF)
            p_all[step, part, :] = p
            return acc + mm(vt[:, part], p)

        out_t = lax.fori_loop(0, n_chunk, value, jnp.zeros((HEAD_DIM, rows), F32))
        srcs, cols = block_of(step)
        o_vm[srcs, :, cols] = out_t.T.astype(BF).reshape(n_src, n_rows, HEAD_DIM)
        return carry

    lax.fori_loop(0, n_step, forward, 0)
    loads[3].wait()
    for off in range(1, n_head):
        remote(do_in.at[row_peer(off)], do_vm.at[from_peer(off)], do_send.at[off - 1], do_recv.at[off - 1], me).wait_recv()

    def row_delta(step, carry):
        prod = read_block(do_vm, step).astype(F32) * read_block(o_vm, step).astype(F32)
        delta_ref[step] = jnp.broadcast_to(jnp.sum(prod.T, axis=0, keepdims=True), (8, rows))
        return carry

    lax.fori_loop(0, n_step, row_delta, 0)
    keep_o = pltpu.make_async_copy(o_vm.at[head_id], o_full.at[:, wide], loc_sem.at[0])
    keep_o.start()
    for off in range(1, n_head):
        row_copy(o_vm, o_full.at[:, wide], o_send, o_recv, off).start()

    dq_base = n_tile * n_rows

    def o_tile(step):
        return pltpu.make_async_copy(wo.at[:, aligned(step * tile, tile)], p_all.at[step], w_sem.at[step])

    def grad_steps(order, low, high):
        off = (2, ahead, behind, 0)[order]
        first, last = order == 0, order == n_seq - 1
        base = lax.rem(seq_id + off, n_seq) * part_keys

        def one(step, carry):
            if last:
                @pl.when(step > 0)
                def _():
                    o_tile(step - 1).start()
            q_blk = read_block(q_vm, step)
            do_blk = read_block(do_vm, step)
            delta = delta_ref[step][0:1, :]
            dq_rows = aligned(dq_base + step * HEAD_DIM, HEAD_DIM)
            acc = None if first else s_buf[dq_rows, :]
            for i in range(part_keys // blk):
                part = aligned(base + i * blk, blk)
                here = pl.ds(i * blk, blk)
                p = p_all[step, part, :]
                dp = mm(v_vm[part, :], do_blk, NT)
                ds = (p.astype(F32) * (dp - delta)).astype(BF)
                dv_acc[order, here, :] += mm(p, do_blk)
                dk_acc[order, here, :] += mm(ds, q_blk)
                add = mm(kt[:, part], ds)
                acc = add if acc is None else acc + add
            if last:
                srcs, cols = block_of(step)
                dq_vm[srcs, :, cols] = (acc * scale).T.astype(BF).reshape(n_src, n_rows, HEAD_DIM)
            else:
                s_buf[dq_rows, :] = acc
            return carry

        lax.fori_loop(low, high, one, 0)

    def clear(order):
        dk_acc[order] = jnp.zeros((part_keys, HEAD_DIM), F32)
        dv_acc[order] = jnp.zeros((part_keys, HEAD_DIM), F32)

    def add_into(acc, order, other):
        def one(i, carry):
            part = aligned(i * n_rows, n_rows)
            acc[order, part, :] += other[part, :]
            return carry
        lax.fori_loop(0, part_keys // n_rows, one, 0)

    early = n_step // 4
    sends = (
        (col_copy(dk_acc.at[0], mid_k, yk_send, yk_recv, 0, ahead), col_copy(dv_acc.at[0], mid_v, yv_send, yv_recv, 0, behind)),
        (col_copy(dk_acc.at[1], rx_k.at[0], yk_send, yk_recv, 1, ahead), col_copy(dv_acc.at[1], rx_v.at[1], yv_send, yv_recv, 2, ahead)),
        (col_copy(dv_acc.at[2], rx_v.at[0], yv_send, yv_recv, 1, behind), col_copy(dk_acc.at[2], rx_k.at[1], yk_send, yk_recv, 2, behind)),
    )
    for order in range(n_seq):
        clear(order)
        if order == 1:
            for copy in sends[0]:
                copy.start()
        if order < 2:
            grad_steps(order, 0, n_step)
            continue
        grad_steps(order, 0, early)
        if order == 2:
            sends[0][0].wait_recv()
            add_into(dk_acc, 1, mid_k)
        else:
            sends[0][1].wait_recv()
            add_into(dv_acc, 2, mid_v)
        sends[order - 1][1].start()
        sends[order - 1][0].start()
        grad_steps(order, early, n_step)
    o_tile(n_step - 1).start()
    dq_full[head_id] = dq_vm[head_id]
    for off in range(1, n_head):
        row_copy(dq_vm, dq_full.at[head_id], dq_send, dq_recv, off).start()
    keep_o.wait()
    for off in range(1, n_head):
        remote(o_vm.at[row_peer(off)], o_full.at[:, aligned(from_peer(off) * width, width)],
               o_send.at[off - 1], o_recv.at[off - 1], me).wait_recv()

    def q_tile(step):
        src = lax.rem(head_id + n_head - step, n_head)
        return pltpu.make_async_copy(wq.at[:, aligned(src * width, width)], p_all.at[step], w_sem.at[step])

    def y_step(step, carry):
        o_tile(step).wait()

        @pl.when(step > 0)
        def _():
            q_tile(step - 1).start()

        y_ref[:, aligned(step * tile, tile)] = mm(o_full[...], p_all[step]).astype(BF)
        return carry

    lax.fori_loop(0, n_tile, y_step, 0)
    q_tile(n_tile - 1).start()
    n_kv = wk.shape[1] // tile
    kv_tiles = [pltpu.make_async_copy(src.at[:, pl.ds(t * tile, tile)], p_all.at[which * n_kv + t], w_sem.at[which * n_kv + t])
                for which, src in enumerate((wk, wv)) for t in range(n_kv)]

    def dx_piece(step, first):
        src = lax.rem(head_id + n_head - step, n_head)
        for e in range(n_tile):
            here = pl.ds(e * n_rows, n_rows)
            add = mm(dq_full[src], p_all[step, e * tile:(e + 1) * tile, :], NT)
            s_buf[here, :] = add if first else s_buf[here, :] + add

    def dx_step(step, carry):
        q_tile(step).wait()
        src = lax.rem(head_id + n_head - step, n_head)
        remote(dq_vm.at[src], dq_full.at[src], dq_send.at[step - 1], dq_recv.at[step - 1], me).wait_recv()
        dx_piece(step, False)
        return carry

    q_tile(0).wait()
    dx_piece(0, True)
    half = n_head // 2
    lax.fori_loop(1, half, dx_step, 0)
    for copy in kv_tiles[:half]:
        copy.start()

    def reduce_own(acc, rx, stage, send, recv, gain):
        for slot, off in ((1, ahead), (2, behind)):
            col_copy(acc.at[0], rx.at[slot - 1], send, recv, slot, off).wait_recv()

        def one(head, carry):
            part = aligned(head * n_rows, n_rows)
            stage[head] = ((acc[n_seq - 1, part, :] + rx[0, part, :] + rx[1, part, :]) * gain).astype(BF)
            return carry

        lax.fori_loop(0, n_head, one, 0)

    reduce_own(dk_acc, rx_k, k_st, yk_send, yk_recv, scale)
    reduce_own(dv_acc, rx_v, v_st, yv_send, yv_recv, 1.0)
    for stage, full, send, recv in ((k_st, dk_full, k_send, k_recv), (v_st, dv_full, v_send, v_recv)):
        for off in range(1, n_head):
            row_copy(stage, full.at[:, slim], send, recv, off).start()
        full[:, slim] = stage[head_id]
    lax.fori_loop(half, n_head, dx_step, 0)
    for copy in kv_tiles[half:]:
        copy.start()
    for stage, full, send, recv in ((k_st, dk_full, k_send, k_recv), (v_st, dv_full, v_send, v_recv)):
        for off in range(1, n_head):
            remote(stage.at[row_peer(off)], full.at[:, aligned(from_peer(off) * HEAD_DIM, HEAD_DIM)],
                   send.at[off - 1], recv.at[off - 1], me).wait_recv()
    for copy in kv_tiles:
        copy.wait()

    def last_step(e, carry):
        part = aligned(e * tile, tile)
        total = s_buf[aligned(e * n_rows, n_rows), :]
        for which, full in enumerate((dk_full, dv_full)):
            for t in range(n_kv):
                total = total + mm(full[:, t * tile:(t + 1) * tile], p_all[which * n_kv + t, part, :], NT)
        dx_ref[:, part] = total.astype(BF)
        return carry

    lax.fori_loop(0, n_tile, last_step, 0)
    for group in sends:
        for copy in group:
            copy.wait_send()
    for off in range(1, n_head):
        row_copy(do_in, do_vm.at[head_id], do_send, do_recv, off).wait_send()
        row_copy(o_vm, o_full.at[:, wide], o_send, o_recv, off).wait_send()
        row_copy(dq_vm, dq_full.at[head_id], dq_send, dq_recv, off).wait_send()
        row_copy(k_st, dk_full.at[:, slim], k_send, k_recv, off).wait_send()
        row_copy(v_st, dv_full.at[:, slim], v_send, v_recv, off).wait_send()


def solution(mesh):
    n_group = mesh.shape["cp"]
    row_spec = P(("dp", "cp"), None)
    full_spec = P(None, None)
    any_spec = pl.BlockSpec(memory_space=pl.ANY)
    vmem_spec = pl.BlockSpec(memory_space=pltpu.VMEM)
    dma = pltpu.SemaphoreType.DMA

    def local_body(x_loc, dy_loc, w_q, w_k, w_v, w_o):
        n_rows, n_model = x_loc.shape
        n_head = w_k.shape[1] // HEAD_DIM
        width = w_q.shape[1] // n_head
        q_group = width // HEAD_DIM
        n_seq = n_group // n_head
        n_keys = n_rows * n_group
        piece = jax.ShapeDtypeStruct((n_head, n_rows, width), BF)
        keys = jax.ShapeDtypeStruct((n_group, n_rows, HEAD_DIM), BF)
        q_all, do_own, k_all, v_all = pl.pallas_call(
            functools.partial(proj_kernel, n_seq, n_head),
            out_shape=(piece, piece, keys, keys),
            in_specs=[vmem_spec, vmem_spec] + [any_spec] * 4,
            out_specs=(any_spec, vmem_spec, any_spec, any_spec),
            scratch_shapes=[pltpu.VMEM((N_SLOT, n_model, width), BF), pltpu.VMEM((N_SLOT, width, n_model), BF),
                            pltpu.VMEM((n_head, n_rows, width), BF),
                            pltpu.VMEM((n_head, n_rows, HEAD_DIM), BF), pltpu.VMEM((n_head, n_rows, HEAD_DIM), BF),
                            dma((N_SLOT,)), dma((N_SLOT,))]
                           + [dma((n_head,))] * 6 + [dma((3,))] * 4 + [dma((3,))],
            compiler_params=pltpu.CompilerParams(collective_id=0, has_side_effects=True, vmem_limit_bytes=VMEM_BYTES),
            name="proj_scatter",
        )(x_loc, dy_loc, w_q, w_k, w_v, w_o)

        rows = max(1, min(n_head, BQ_ROWS // n_rows)) * n_rows
        n_step = q_group * n_head * n_rows // rows
        part_keys = n_keys // n_seq
        acts = pltpu.VMEM((n_head, n_rows, width), BF)
        flat = pltpu.VMEM((n_rows, n_head * width), BF)
        head_keys = pltpu.VMEM((n_keys, HEAD_DIM), BF)
        head_keys_t = pltpu.VMEM((HEAD_DIM, n_keys), BF)
        sums = pltpu.VMEM((n_seq, part_keys, HEAD_DIM), F32)
        mid = pltpu.VMEM((part_keys, HEAD_DIM), F32)
        pair = pltpu.VMEM((2, part_keys, HEAD_DIM), F32)
        stage = pltpu.VMEM((n_head, n_rows, HEAD_DIM), BF)
        slim = pltpu.VMEM((n_rows, n_head * HEAD_DIM), BF)
        y_loc, dx_loc = pl.pallas_call(
            functools.partial(main_kernel, n_seq, n_head),
            out_shape=(jax.ShapeDtypeStruct((n_rows, n_model), BF), jax.ShapeDtypeStruct((n_rows, n_model), BF)),
            in_specs=[any_spec] * 8,
            out_specs=(vmem_spec, vmem_spec),
            scratch_shapes=[pltpu.VMEM((n_step, n_keys, rows), BF), pltpu.VMEM((n_keys, rows), F32), acts,
                            head_keys, head_keys, head_keys_t, head_keys_t, acts, acts, acts, flat, acts,
                            pltpu.VMEM((n_step, 8, rows), F32), sums, sums, mid, mid, pair, pair, stage, stage, slim, slim,
                            dma((4,)), dma((n_step,)), dma((1,))] + [dma((n_head - 1,))] * 10 + [dma((3,))] * 4,
            compiler_params=pltpu.CompilerParams(collective_id=1, has_side_effects=True, vmem_limit_bytes=VMEM_MAIN),
            name="attend_out",
        )(q_all, do_own, k_all.reshape(n_keys, HEAD_DIM), v_all.reshape(n_keys, HEAD_DIM), w_q, w_k, w_v, w_o)
        return y_loc, dx_loc

    return jax.shard_map(local_body, mesh=mesh,
                         in_specs=(row_spec, row_spec, full_spec, full_spec, full_spec, full_spec),
                         out_specs=(row_spec, row_spec), check_vma=False)
```

```python
import functools

import jax
import jax.numpy as jnp
from jax import lax
from jax.experimental import pallas as pl
from jax.experimental.pallas import tpu as pltpu
from jax.sharding import PartitionSpec as P

HEAD_DIM = 128
LOG2E = 1.4426950408889634
N_SLOT = 4
BQ_ROWS = 512
UC_ROWS = 512
SCORE_ROWS = 2048
EXP_ROWS = 1024
SUB_ROWS = 256
VMEM_BYTES = 62 * 1024 * 1024
VMEM_MAIN = 67000000
MESH_ID = pl.DeviceIdType.MESH
BF = jnp.bfloat16
F32 = jnp.float32
NT = (((1,), (1,)), ((), ()))
NN = (((1,), (0,)), ((), ()))


def mm(a, b, dims=NN):
    return lax.dot_general(a, b, dims, preferred_element_type=F32)


def aligned(start, size):
    return pl.ds(pl.multiple_of(start, size), size)


def entry_barrier(seq_id, head_id, n_seq, n_head):
    sem = pltpu.get_barrier_semaphore()
    for off in range(1, n_head):
        peer = seq_id * n_head + lax.rem(head_id + off, n_head)
        pl.semaphore_signal(sem, inc=1, device_id={"cp": peer}, device_id_type=MESH_ID)
    for off in range(1, n_seq):
        peer = lax.rem(seq_id + off, n_seq) * n_head + head_id
        pl.semaphore_signal(sem, inc=1, device_id={"cp": peer}, device_id_type=MESH_ID)
    pl.semaphore_wait(sem, n_head + n_seq - 2)


def remote(src, dst, send, recv, peer):
    return pltpu.make_async_remote_copy(src_ref=src, dst_ref=dst, send_sem=send, recv_sem=recv,
                                        device_id={"cp": peer}, device_id_type=MESH_ID)


def proj_kernel(n_seq, n_head, x_ref, dy_ref, wq, wk, wv, wo, q_out, do_out, k_out, v_out,
                wbuf, obuf, q_st, k_st, v_st, w_sem, o_sem,
                q_send, q_recv, k_send, k_recv, v_send, v_recv,
                ky_send, ky_recv, vy_send, vy_recv, loc_sem):
    me = lax.axis_index("cp")
    head_id = lax.rem(me, n_head)
    seq_id = lax.div(me, n_head)
    width = q_st.shape[2]
    per_tile = width // HEAD_DIM
    n_kv = n_head // per_tile
    n_pre = N_SLOT - 1

    def dest(step):
        return lax.rem(head_id + 1 + step, n_head)

    def col_tile(tile):
        slot = tile % N_SLOT
        if tile < n_kv:
            src = wk.at[:, pl.ds(tile * width, width)]
        elif tile < 2 * n_kv:
            src = wv.at[:, pl.ds((tile - n_kv) * width, width)]
        else:
            src = wq.at[:, aligned(dest(tile - 2 * n_kv) * width, width)]
        return pltpu.make_async_copy(src, wbuf.at[slot], w_sem.at[slot])

    def q_tile(step):
        slot = lax.rem(step + 2 * n_kv, N_SLOT)
        return pltpu.make_async_copy(wq.at[:, aligned(dest(step) * width, width)], wbuf.at[slot], w_sem.at[slot])

    def o_tile(step):
        slot = lax.rem(step, N_SLOT)
        return pltpu.make_async_copy(wo.at[aligned(dest(step) * width, width), :], obuf.at[slot], o_sem.at[slot])

    for tile in range(n_pre):
        col_tile(tile).start()
    entry_barrier(seq_id, head_id, n_seq, n_head)

    def kv_send(tile):
        stage, out, send, recv, loc = (k_st, k_out, k_send, k_recv, 0) if tile < n_kv else (v_st, v_out, v_send, v_recv, 1)
        for sub in range(per_tile):
            head = (tile % n_kv) * per_tile + sub

            @pl.when(head != head_id)
            def _():
                remote(stage.at[head], out.at[me], send.at[head], recv.at[head_id], seq_id * n_head + head).start()

            @pl.when(head == head_id)
            def _():
                pltpu.make_async_copy(stage.at[head], out.at[me], loc_sem.at[loc]).start()

    for tile in range(2 * n_kv):
        col_tile(tile).wait()
        if tile >= 1:
            kv_send(tile - 1)
        col_tile(tile + n_pre).start()
        prod = mm(x_ref[...], wbuf[tile % N_SLOT]).astype(BF)
        stage = k_st if tile < n_kv else v_st
        for sub in range(per_tile):
            stage[(tile % n_kv) * per_tile + sub] = prod[:, sub * HEAD_DIM:(sub + 1) * HEAD_DIM]

    def send_piece(stage, out, send, recv, loc, step):
        head = dest(step)

        @pl.when(step < n_head - 1)
        def _():
            remote(stage.at[head], out.at[head_id], send.at[head], recv.at[head_id], seq_id * n_head + head).start()

        @pl.when(step == n_head - 1)
        def _():
            pltpu.make_async_copy(stage.at[head], out.at[head_id], loc_sem.at[loc]).start()

    def row_copy(stage, out, send, recv, off, dst_base):
        src = lax.rem(head_id + off, n_head)
        return remote(stage.at[src], out.at[dst_base + src], send.at[src], recv.at[src], seq_id * n_head + src)

    ahead, behind = 1, n_seq - 1

    def seq_copy(out, send, recv, slot, origin, off):
        rows = pl.ds(lax.rem(seq_id + origin, n_seq) * n_head, n_head)
        peer = lax.rem(seq_id + off, n_seq) * n_head + head_id
        return remote(out.at[rows], out.at[rows], send.at[slot], recv.at[slot], peer)

    relays = ((k_out, ky_send, ky_recv, ahead), (v_out, vy_send, vy_recv, behind))

    def relay(which):
        out, send, recv, off = relays[which]
        stage, x_send, x_recv = ((k_st, k_send, k_recv), (v_st, v_send, v_recv))[which]
        for place in range(1, n_head):
            row_copy(stage, out, x_send, x_recv, place, seq_id * n_head).wait_recv()
        pltpu.make_async_copy(stage.at[head_id], out.at[me], loc_sem.at[which]).wait()
        seq_copy(out, send, recv, 0, 0, off).start()
        seq_copy(out, send, recv, 1, 0, n_seq - off).start()

    def forward(which):
        out, send, recv, off = relays[which]
        seq_copy(out, send, recv, 0, n_seq - off, off).wait_recv()
        seq_copy(out, send, recv, 2, n_seq - off, off).start()

    relay_steps = (n_head // 4 - 1, (3 * n_head) // 8)

    def q_step(step, carry):
        q_tile(step).wait()

        @pl.when(step == 0)
        def _():
            kv_send(2 * n_kv - 1)

        @pl.when(step > 0)
        def _():
            send_piece(q_st, q_out, q_send, q_recv, 2, step - 1)

        @pl.when(step + n_pre < n_head)
        def _():
            q_tile(step + n_pre).start()

        @pl.when(step + n_pre >= n_head)
        def _():
            o_tile(step + n_pre - n_head).start()

        for which in range(2):
            @pl.when(step == relay_steps[which])
            def _():
                relay(which)

        slot = lax.rem(step + 2 * n_kv, N_SLOT)
        q_st[dest(step)] = mm(x_ref[...], wbuf[slot]).astype(BF)
        return carry

    lax.fori_loop(0, n_head, q_step, 0)

    forward_steps = (0, n_head // 4)

    def do_step(step, carry):
        o_tile(step).wait()

        @pl.when(step == 0)
        def _():
            send_piece(q_st, q_out, q_send, q_recv, 2, n_head - 1)

        for which in range(2):
            @pl.when(step == forward_steps[which])
            def _():
                forward(which)

        @pl.when(step + n_pre < n_head)
        def _():
            o_tile(step + n_pre).start()

        do_out[dest(step)] = mm(dy_ref[...], obuf[lax.rem(step, N_SLOT)], NT).astype(BF)
        return carry

    lax.fori_loop(0, n_head, do_step, 0)
    for off in range(1, n_head):
        row_copy(q_st, q_out, q_send, q_recv, off, 0).wait()
        row_copy(k_st, k_out, k_send, k_recv, off, seq_id * n_head).wait_send()
        row_copy(v_st, v_out, v_send, v_recv, off, seq_id * n_head).wait_send()
    pltpu.make_async_copy(q_st.at[head_id], q_out.at[head_id], loc_sem.at[2]).wait()
    for out, send, recv, off in relays:
        seq_copy(out, send, recv, 0, 0, off).wait_send()
        seq_copy(out, send, recv, 1, 0, n_seq - off).wait_send()
        seq_copy(out, send, recv, 2, n_seq - off, off).wait_send()
        seq_copy(out, send, recv, 1, off, off).wait_recv()
        seq_copy(out, send, recv, 2, 2, off).wait_recv()


def main_kernel(n_seq, n_head, q_in, do_in, k_in, v_in, wq, wk, wv, wo, y_ref, dx_ref,
                p_all, s_buf, q_vm, k_vm, v_vm, kt, vt, do_vm, o_vm, dq_vm, o_full, dq_full, delta_ref,
                dk_acc, dv_acc, mid_k, mid_v, rx_k, rx_v, k_st, v_st, dk_full, dv_full,
                in_sem, w_sem, loc_sem, do_send, do_recv, o_send, o_recv, dq_send, dq_recv,
                k_send, k_recv, v_send, v_recv, yk_send, yk_recv, yv_send, yv_recv):
    me = lax.axis_index("cp")
    head_id = lax.rem(me, n_head)
    seq_id = lax.div(me, n_head)
    n_keys = k_vm.shape[0]
    n_rows, width = q_vm.shape[1], q_vm.shape[2]
    q_group = width // HEAD_DIM
    n_step, _, rows = p_all.shape
    n_src = rows // n_rows
    n_blk = n_step // q_group
    tile = p_all.shape[2]
    n_tile = y_ref.shape[1] // tile
    blk = min(UC_ROWS, n_keys // n_seq)
    n_chunk = n_keys // blk
    sub = SUB_ROWS
    part_keys = n_keys // n_seq
    scale = HEAD_DIM ** -0.5
    gain = scale * LOG2E
    ahead, behind = 1, n_seq - 1

    def row_peer(off):
        return lax.rem(head_id + off, n_head)

    def row_copy(src, dst, send, recv, off):
        return remote(src.at[row_peer(off)], dst, send.at[off - 1], recv.at[off - 1], seq_id * n_head + row_peer(off))

    def col_copy(src, dst, send, recv, slot, off):
        return remote(src, dst, send.at[slot], recv.at[slot], lax.rem(seq_id + off, n_seq) * n_head + head_id)

    wide = aligned(head_id * width, width)
    slim = aligned(head_id * HEAD_DIM, HEAD_DIM)

    def from_peer(off):
        return row_peer(n_head - off)

    loads = (pltpu.make_async_copy(k_in, k_vm, in_sem.at[0]), pltpu.make_async_copy(q_in, q_vm, in_sem.at[1]),
             pltpu.make_async_copy(v_in, v_vm, in_sem.at[2]),
             pltpu.make_async_copy(do_in.at[head_id], do_vm.at[head_id], in_sem.at[3]))
    for copy in loads:
        copy.start()
    entry_barrier(seq_id, head_id, n_seq, n_head)
    for off in range(1, n_head):
        row_copy(do_in, do_vm.at[head_id], do_send, do_recv, off).start()
    for copy in loads[:3]:
        copy.wait()

    def prep(i, carry):
        part = aligned(i * blk, blk)
        kt[:, part] = k_vm[part, :].astype(F32).T.astype(BF)
        vt[:, part] = v_vm[part, :].astype(F32).T.astype(BF)
        return carry

    lax.fori_loop(0, n_chunk, prep, 0)

    def block_of(step):
        return pl.ds(lax.rem(step, n_blk) * n_src, n_src), aligned(lax.div(step, n_blk) * HEAD_DIM, HEAD_DIM)

    def read_block(ref, step):
        srcs, cols = block_of(step)
        return ref[srcs, :, cols].reshape(rows, HEAD_DIM)

    def forward(step, carry):
        q_blk = read_block(q_vm, step)

        def score(i, top):
            for u in range(SCORE_ROWS // sub):
                part = aligned(i * SCORE_ROWS + u * sub, sub)
                s = mm(k_vm[part, :], q_blk, NT)
                s_buf[part, :] = s
                top = jnp.maximum(top, jnp.max(s.reshape(sub // 8, 8, rows), axis=0))
            return top

        top = lax.fori_loop(0, n_keys // SCORE_ROWS, score, jnp.full((8, rows), -jnp.inf, F32))
        top = jnp.max(top, axis=0, keepdims=True)

        def expo(i, tot):
            for u in range(EXP_ROWS // sub):
                part = aligned(i * EXP_ROWS + u * sub, sub)
                e = jnp.exp2((s_buf[part, :] - top) * gain)
                s_buf[part, :] = e
                tot = tot + jnp.sum(e.reshape(sub // 8, 8, rows), axis=0)
            return tot

        tot = lax.fori_loop(0, n_keys // EXP_ROWS, expo, jnp.zeros((8, rows), F32))
        inv = 1.0 / jnp.sum(tot, axis=0, keepdims=True)

        out_t = None
        for u in range(n_keys // sub):
            part = pl.ds(u * sub, sub)
            p = (s_buf[part, :] * inv).astype(BF)
            p_all[step, part, :] = p
            one = mm(vt[:, part], p)
            out_t = one if out_t is None else out_t + one
        srcs, cols = block_of(step)
        o_vm[srcs, :, cols] = out_t.T.astype(BF).reshape(n_src, n_rows, HEAD_DIM)
        return carry

    lax.fori_loop(0, n_step, forward, 0)
    loads[3].wait()
    for off in range(1, n_head):
        remote(do_in.at[row_peer(off)], do_vm.at[from_peer(off)], do_send.at[off - 1], do_recv.at[off - 1], me).wait_recv()

    def row_delta(step, carry):
        prod = read_block(do_vm, step).astype(F32) * read_block(o_vm, step).astype(F32)
        delta_ref[step] = jnp.broadcast_to(jnp.sum(prod.T, axis=0, keepdims=True), (8, rows))
        return carry

    lax.fori_loop(0, n_step, row_delta, 0)
    keep_o = pltpu.make_async_copy(o_vm.at[head_id], o_full.at[:, wide], loc_sem.at[0])
    keep_o.start()
    for off in range(1, n_head):
        row_copy(o_vm, o_full.at[:, wide], o_send, o_recv, off).start()

    dq_base = n_tile * n_rows

    def o_tile(step):
        return pltpu.make_async_copy(wo.at[:, aligned(step * tile, tile)], p_all.at[step], w_sem.at[step])

    def grad_steps(order, low, high):
        off = (2, ahead, behind, 0)[order]
        first, last = order == 0, order == n_seq - 1
        base = lax.rem(seq_id + off, n_seq) * part_keys

        def one(step, carry):
            if last:
                @pl.when(step > 0)
                def _():
                    o_tile(step - 1).start()
            q_blk = read_block(q_vm, step)
            do_blk = read_block(do_vm, step)
            delta = delta_ref[step][0:1, :]
            dq_rows = aligned(dq_base + step * HEAD_DIM, HEAD_DIM)
            acc = None if first else s_buf[dq_rows, :]
            for i in range(part_keys // blk):
                part = aligned(base + i * blk, blk)
                here = pl.ds(i * blk, blk)
                p = p_all[step, part, :]
                dp = mm(v_vm[part, :], do_blk, NT)
                ds = (p.astype(F32) * (dp - delta)).astype(BF)
                dv_acc[order, here, :] += mm(p, do_blk)
                dk_acc[order, here, :] += mm(ds, q_blk)
                add = mm(kt[:, part], ds)
                acc = add if acc is None else acc + add
            if last:
                srcs, cols = block_of(step)
                dq_vm[srcs, :, cols] = (acc * scale).T.astype(BF).reshape(n_src, n_rows, HEAD_DIM)
            else:
                s_buf[dq_rows, :] = acc
            return carry

        lax.fori_loop(low, high, one, 0)

    def clear(order):
        dk_acc[order] = jnp.zeros((part_keys, HEAD_DIM), F32)
        dv_acc[order] = jnp.zeros((part_keys, HEAD_DIM), F32)

    def add_into(acc, order, other):
        def one(i, carry):
            part = aligned(i * n_rows, n_rows)
            acc[order, part, :] += other[part, :]
            return carry
        lax.fori_loop(0, part_keys // n_rows, one, 0)

    early = n_step // 4
    sends = (
        (col_copy(dk_acc.at[0], mid_k, yk_send, yk_recv, 0, ahead), col_copy(dv_acc.at[0], mid_v, yv_send, yv_recv, 0, behind)),
        (col_copy(dk_acc.at[1], rx_k.at[0], yk_send, yk_recv, 1, ahead), col_copy(dv_acc.at[1], rx_v.at[1], yv_send, yv_recv, 2, ahead)),
        (col_copy(dv_acc.at[2], rx_v.at[0], yv_send, yv_recv, 1, behind), col_copy(dk_acc.at[2], rx_k.at[1], yk_send, yk_recv, 2, behind)),
    )
    for order in range(n_seq):
        clear(order)
        if order == 1:
            for copy in sends[0]:
                copy.start()
        if order < 2:
            grad_steps(order, 0, n_step)
            continue
        grad_steps(order, 0, early)
        if order == 2:
            sends[0][0].wait_recv()
            add_into(dk_acc, 1, mid_k)
        else:
            sends[0][1].wait_recv()
            add_into(dv_acc, 2, mid_v)
        sends[order - 1][1].start()
        sends[order - 1][0].start()
        grad_steps(order, early, n_step)
    o_tile(n_step - 1).start()
    dq_full[head_id] = dq_vm[head_id]
    for off in range(1, n_head):
        row_copy(dq_vm, dq_full.at[head_id], dq_send, dq_recv, off).start()
    keep_o.wait()
    for off in range(1, n_head):
        remote(o_vm.at[row_peer(off)], o_full.at[:, aligned(from_peer(off) * width, width)],
               o_send.at[off - 1], o_recv.at[off - 1], me).wait_recv()

    def q_tile(step):
        src = lax.rem(head_id + n_head - step, n_head)
        return pltpu.make_async_copy(wq.at[:, aligned(src * width, width)], p_all.at[step], w_sem.at[step])

    def y_step(step, carry):
        o_tile(step).wait()

        @pl.when(step > 0)
        def _():
            q_tile(step - 1).start()

        y_ref[:, aligned(step * tile, tile)] = mm(o_full[...], p_all[step]).astype(BF)
        return carry

    lax.fori_loop(0, n_tile, y_step, 0)
    q_tile(n_tile - 1).start()
    n_kv = wk.shape[1] // tile
    kv_tiles = [pltpu.make_async_copy(src.at[:, pl.ds(t * tile, tile)], p_all.at[which * n_kv + t], w_sem.at[which * n_kv + t])
                for which, src in enumerate((wk, wv)) for t in range(n_kv)]

    def dx_piece(step, first):
        src = lax.rem(head_id + n_head - step, n_head)
        for e in range(n_tile):
            here = pl.ds(e * n_rows, n_rows)
            add = mm(dq_full[src], p_all[step, e * tile:(e + 1) * tile, :], NT)
            s_buf[here, :] = add if first else s_buf[here, :] + add

    def dx_step(step, carry):
        q_tile(step).wait()
        src = lax.rem(head_id + n_head - step, n_head)
        remote(dq_vm.at[src], dq_full.at[src], dq_send.at[step - 1], dq_recv.at[step - 1], me).wait_recv()
        dx_piece(step, False)
        return carry

    q_tile(0).wait()
    dx_piece(0, True)
    half = n_head // 2
    lax.fori_loop(1, half, dx_step, 0)
    for copy in kv_tiles[:half]:
        copy.start()

    def reduce_own(acc, rx, stage, send, recv, gain):
        for slot, off in ((1, ahead), (2, behind)):
            col_copy(acc.at[0], rx.at[slot - 1], send, recv, slot, off).wait_recv()

        def one(head, carry):
            part = aligned(head * n_rows, n_rows)
            stage[head] = ((acc[n_seq - 1, part, :] + rx[0, part, :] + rx[1, part, :]) * gain).astype(BF)
            return carry

        lax.fori_loop(0, n_head, one, 0)

    reduce_own(dk_acc, rx_k, k_st, yk_send, yk_recv, scale)
    reduce_own(dv_acc, rx_v, v_st, yv_send, yv_recv, 1.0)
    for stage, full, send, recv in ((k_st, dk_full, k_send, k_recv), (v_st, dv_full, v_send, v_recv)):
        for off in range(1, n_head):
            row_copy(stage, full.at[:, slim], send, recv, off).start()
        full[:, slim] = stage[head_id]
    lax.fori_loop(half, n_head, dx_step, 0)
    for copy in kv_tiles[half:]:
        copy.start()
    for stage, full, send, recv in ((k_st, dk_full, k_send, k_recv), (v_st, dv_full, v_send, v_recv)):
        for off in range(1, n_head):
            remote(stage.at[row_peer(off)], full.at[:, aligned(from_peer(off) * HEAD_DIM, HEAD_DIM)],
                   send.at[off - 1], recv.at[off - 1], me).wait_recv()
    for copy in kv_tiles:
        copy.wait()

    def last_step(e, carry):
        part = aligned(e * tile, tile)
        total = s_buf[aligned(e * n_rows, n_rows), :]
        for which, full in enumerate((dk_full, dv_full)):
            for t in range(n_kv):
                total = total + mm(full[:, t * tile:(t + 1) * tile], p_all[which * n_kv + t, part, :], NT)
        dx_ref[:, part] = total.astype(BF)
        return carry

    lax.fori_loop(0, n_tile, last_step, 0)
    for group in sends:
        for copy in group:
            copy.wait_send()
    for off in range(1, n_head):
        row_copy(do_in, do_vm.at[head_id], do_send, do_recv, off).wait_send()
        row_copy(o_vm, o_full.at[:, wide], o_send, o_recv, off).wait_send()
        row_copy(dq_vm, dq_full.at[head_id], dq_send, dq_recv, off).wait_send()
        row_copy(k_st, dk_full.at[:, slim], k_send, k_recv, off).wait_send()
        row_copy(v_st, dv_full.at[:, slim], v_send, v_recv, off).wait_send()


def copy_kernel(n_cut, y_in, dx_in, y_out, dx_out, buf, in_sem, out_sem):
    rows = y_in.shape[0] // n_cut
    cuts = [(src, dst, slot, pl.ds(cut * rows, rows), slot * n_cut + cut)
            for cut in range(n_cut) for slot, (src, dst) in enumerate(((y_in, y_out), (dx_in, dx_out)))]
    ins = [pltpu.make_async_copy(src.at[part], buf.at[slot, part], in_sem.at[sem]) for src, dst, slot, part, sem in cuts]
    outs = [pltpu.make_async_copy(buf.at[slot, part], dst.at[part], out_sem.at[sem]) for src, dst, slot, part, sem in cuts]
    for copy in ins:
        copy.start()
    for copy, later in zip(ins, outs):
        copy.wait()
        later.start()
    for copy in outs:
        copy.wait()


def solution(mesh):
    n_group = mesh.shape["cp"]
    row_spec = P(("dp", "cp"), None)
    full_spec = P(None, None)
    any_spec = pl.BlockSpec(memory_space=pl.ANY)
    vmem_spec = pl.BlockSpec(memory_space=pltpu.VMEM)
    dma = pltpu.SemaphoreType.DMA

    def local_body(x_loc, dy_loc, w_q, w_k, w_v, w_o):
        n_rows, n_model = x_loc.shape
        n_head = w_k.shape[1] // HEAD_DIM
        width = w_q.shape[1] // n_head
        q_group = width // HEAD_DIM
        n_seq = n_group // n_head
        n_keys = n_rows * n_group
        piece = jax.ShapeDtypeStruct((n_head, n_rows, width), BF)
        keys = jax.ShapeDtypeStruct((n_group, n_rows, HEAD_DIM), BF)
        q_all, do_own, k_all, v_all = pl.pallas_call(
            functools.partial(proj_kernel, n_seq, n_head),
            out_shape=(piece, piece, keys, keys),
            in_specs=[vmem_spec, vmem_spec] + [any_spec] * 4,
            out_specs=(any_spec, vmem_spec, any_spec, any_spec),
            scratch_shapes=[pltpu.VMEM((N_SLOT, n_model, width), BF), pltpu.VMEM((N_SLOT, width, n_model), BF),
                            pltpu.VMEM((n_head, n_rows, width), BF),
                            pltpu.VMEM((n_head, n_rows, HEAD_DIM), BF), pltpu.VMEM((n_head, n_rows, HEAD_DIM), BF),
                            dma((N_SLOT,)), dma((N_SLOT,))]
                           + [dma((n_head,))] * 6 + [dma((3,))] * 4 + [dma((3,))],
            compiler_params=pltpu.CompilerParams(collective_id=0, has_side_effects=True, vmem_limit_bytes=VMEM_BYTES),
            name="proj_scatter",
        )(x_loc, dy_loc, w_q, w_k, w_v, w_o)

        rows = max(1, min(n_head, BQ_ROWS // n_rows)) * n_rows
        n_step = q_group * n_head * n_rows // rows
        part_keys = n_keys // n_seq
        acts = pltpu.VMEM((n_head, n_rows, width), BF)
        flat = pltpu.VMEM((n_rows, n_head * width), BF)
        head_keys = pltpu.VMEM((n_keys, HEAD_DIM), BF)
        head_keys_t = pltpu.VMEM((HEAD_DIM, n_keys), BF)
        sums = pltpu.VMEM((n_seq, part_keys, HEAD_DIM), F32)
        mid = pltpu.VMEM((part_keys, HEAD_DIM), F32)
        pair = pltpu.VMEM((2, part_keys, HEAD_DIM), F32)
        stage = pltpu.VMEM((n_head, n_rows, HEAD_DIM), BF)
        slim = pltpu.VMEM((n_rows, n_head * HEAD_DIM), BF)
        y_loc, dx_loc = pl.pallas_call(
            functools.partial(main_kernel, n_seq, n_head),
            out_shape=(jax.ShapeDtypeStruct((n_rows, n_model), BF), jax.ShapeDtypeStruct((n_rows, n_model), BF)),
            in_specs=[any_spec] * 8,
            out_specs=(vmem_spec, vmem_spec),
            scratch_shapes=[pltpu.VMEM((n_step, n_keys, rows), BF), pltpu.VMEM((n_keys, rows), F32), acts,
                            head_keys, head_keys, head_keys_t, head_keys_t, acts, acts, acts, flat, acts,
                            pltpu.VMEM((n_step, 8, rows), F32), sums, sums, mid, mid, pair, pair, stage, stage, slim, slim,
                            dma((4,)), dma((n_step,)), dma((1,))] + [dma((n_head - 1,))] * 10 + [dma((3,))] * 4,
            compiler_params=pltpu.CompilerParams(collective_id=1, has_side_effects=True, vmem_limit_bytes=VMEM_MAIN),
            name="attend_out",
        )(q_all, do_own, k_all.reshape(n_keys, HEAD_DIM), v_all.reshape(n_keys, HEAD_DIM), w_q, w_k, w_v, w_o)
        n_cut = 4
        return pl.pallas_call(
            functools.partial(copy_kernel, n_cut),
            out_shape=(jax.ShapeDtypeStruct((n_rows, n_model), BF), jax.ShapeDtypeStruct((n_rows, n_model), BF)),
            in_specs=[any_spec] * 2,
            out_specs=(any_spec, any_spec),
            scratch_shapes=[pltpu.VMEM((2, n_rows, n_model), BF), dma((2 * n_cut,)), dma((2 * n_cut,))],
            name="copy_out",
        )(y_loc, dx_loc)

    return jax.shard_map(local_body, mesh=mesh,
                         in_specs=(row_spec, row_spec, full_spec, full_spec, full_spec, full_spec),
                         out_specs=(row_spec, row_spec), check_vma=False)
```
